32 devices in a mesh: section: 4 (over y, x), dp: 8 (over z, core).
Axes of the slice: x: 2, y: 2, z: 4, core: 2. Of those that a mesh axis runs over, the one named last changes fastest.
Arguments:
- inputs: bfloat16 [16, 128, 3072], P('dp'), may hold values from -6 to 6
- sample_ids: int32 [8, 2], P('dp'), may hold values from 0 to 1, each once within a row
- stored: bfloat16 [4, 2, 16, 128, 3072], P('section', None, 'dp'), may hold values from -4 to 4, as said below
- weight: bfloat16 [4, 3072, 3072], P('section'), may hold values from -0.109375 to 0.109375
- norm_gain: float32 [4, 3072], P('section'), may hold values from 0.1 to 1.9
Outputs:
- section_outputs: bfloat16 [4, 16, 128, 3072], P('section', 'dp')
- weight_grads: bfloat16 [4, 3072, 3072], P('section', 'dp')
The draws below stay inside these ranges and needn't reach their ends.
Inputs may be any that keep to these rules, and one draw needn't show every extreme that they name: `sample_ids`: each row names each of the replica's 2 samples once. `stored`: copy 0 of section s equals copy 1 of section s - 1, and copy 0 of section 0 equals copy 1 of the last section.
All inputs are finite; a program needn't handle non-finite values.
Results may differ from the reference program's by a relative error of at most 0.024.
Values may be sent and summed in bfloat16 or wider, within the bound.
A program may use at most 192 MiB of HBM per device.

```python
import math
import jax
import jax.numpy as jnp
from jax import lax

D = 3072
TOK = 128
MB = 2
N_SECTION = 4
N_DP = 8


def draw_stored(key, part):
    full_shape = (N_SECTION, N_DP * MB, TOK, D)
    base_draw = jnp.clip(jax.random.normal(key, full_shape, jnp.float32), -4.0, 4.0)
    return jnp.stack([jnp.roll(base_draw, 1, axis=0), base_draw], axis=1).astype(jnp.bfloat16)


def level_of(key, extent, shards, smallest, high):
    def one(position, blocks):
        heights = jax.random.uniform(jax.random.fold_in(jax.random.fold_in(key, 6), position), (blocks,), jnp.float32, smallest / len(shards), high / len(shards))
        return jnp.repeat(jnp.exp(heights), extent[position] // blocks).reshape((-1,) + (1,) * (len(extent) - position - 1))

    factor_of = one(*shards[0])
    for cut in shards[1:]:
        factor_of = factor_of * one(*cut)
    return factor_of


def noise(rng, extent, deviation, limit, shards=(), kind=jnp.bfloat16):
    values = deviation * jax.random.normal(rng, extent, jnp.float32)
    if shards:
        values = values * level_of(rng, extent, shards, -0.22, 0.18)
    return jnp.clip(values, -limit, limit).astype(kind)


def setup_inputs(seed: int = 0) -> dict:
    keys = jax.random.split(jax.random.key(seed), 6)
    inputs = noise(keys[0], (N_DP * MB, TOK, D), 1.0, 6.0, ((0, 8),))
    sample_ids = jax.vmap(lambda own: jax.random.permutation(own, MB))(jax.random.split(keys[1], N_DP)).reshape((N_DP, MB)).astype(jnp.int32)
    stored = draw_stored(jax.random.fold_in(keys[5], 71), 0)
    weight = noise(keys[3], (N_SECTION, D, D), D ** -0.5, 0.109375, ((0, 4),))
    norm_gain = jnp.clip(1.0 + 0.18 * jax.random.normal(keys[4], (N_SECTION, D), jnp.float32), 0.1, 1.9)
    return {"inputs": inputs, "sample_ids": sample_ids, "stored": stored, "weight": weight, "norm_gain": norm_gain}


epsilon = 1e-05
delta_bound = 2.0

def activate(values):
    return jax.nn.gelu(values, approximate=False)

def normalize(state, norm_gain):
    average = lax.optimization_barrier(jnp.mean(state, axis=-1, keepdims=True))
    centred = state - average
    variance = lax.optimization_barrier(jnp.mean(centred * centred, axis=-1, keepdims=True))
    return centred * lax.rsqrt(variance + epsilon) * norm_gain

def reference(inputs, sample_ids, stored, weight, norm_gain):
    replica_base = jnp.arange(N_DP, dtype=jnp.int32)[:, None] * MB
    flat_ids = (replica_base + sample_ids.astype(jnp.int32)).reshape(-1).astype(jnp.int32)
    state = inputs.astype(jnp.float32)
    results = []
    stashed = []
    result = state
    for layer_num in range(N_SECTION):
        normed = normalize(state, norm_gain[layer_num]).astype(jnp.bfloat16)
        preact = jnp.dot(normed.reshape(-1, D), weight[layer_num], preferred_element_type=jnp.float32).reshape(state.shape)
        result = state + activate(preact)
        stashed.append((state, normed, preact))
        results.append(result.astype(jnp.bfloat16))
        if layer_num + 1 < N_SECTION:
            sent_copy = stored[layer_num, 1][flat_ids].astype(jnp.float32)
            kept_copy = stored[layer_num + 1, 0][flat_ids].astype(jnp.float32)
            clipped = jnp.clip(result - sent_copy, -delta_bound, delta_bound).astype(jnp.bfloat16)
            clipped = lax.optimization_barrier(clipped)
            state = kept_copy + clipped.astype(jnp.float32)
    loss_scale = 1.0 / math.sqrt(N_DP * MB * TOK)
    upstream = result * loss_scale
    weight_grads = [None] * N_SECTION

    def add_replica(total, operands):
        normed_rows, grad_rows = operands
        replica_sum = jnp.dot(normed_rows.T, grad_rows, preferred_element_type=jnp.float32).astype(jnp.bfloat16)
        replica_sum = lax.optimization_barrier(replica_sum)
        return (total + replica_sum.astype(jnp.float32), None)
    for layer_num in range(N_SECTION - 1, -1, -1):
        state, normed, preact = stashed[layer_num]
        grad_pre = jax.vjp(activate, preact)[1](upstream)[0].astype(jnp.bfloat16)
        normed_split = normed.reshape(N_DP, MB * TOK, D)
        grad_split = grad_pre.reshape(N_DP, MB * TOK, D)
        total, unused = lax.scan(add_replica, jnp.zeros((D, D), jnp.float32), (normed_split, grad_split))
        weight_grads[layer_num] = total.astype(jnp.bfloat16)
        grad_normed = jnp.dot(grad_pre.reshape(-1, D), weight[layer_num].T, preferred_element_type=jnp.float32).reshape(state.shape)
        gain_here = norm_gain[layer_num]
        grad_state = upstream + jax.vjp(lambda values: normalize(values, gain_here), state)[1](grad_normed)[0]
        sent = lax.optimization_barrier(grad_state.astype(jnp.bfloat16))
        upstream = sent.astype(jnp.float32)
    return (jnp.stack(results), jnp.stack(weight_grads))
```

```python
from contextlib import nullcontext
from functools import partial
import math

import jax
import jax.numpy as jnp
from jax import lax
from jax.experimental import pallas as pl
from jax.experimental.pallas import tpu as pltpu
from jax.sharding import PartitionSpec as P

epsilon = 1e-05
delta_bound = 2.0


def from_behind(shard, axis, by):
    length = lax.axis_size(axis)
    pairs = [(i, i + by) for i in range(length) if 0 <= i + by < length]
    return lax.ppermute(shard, axis, pairs)


def activate(values):
    return jax.nn.gelu(values, approximate=False)


def normalize(state, norm_gain):
    average = jnp.mean(state, axis=-1, keepdims=True)
    centred = state - average
    variance = jnp.mean(centred * centred, axis=-1, keepdims=True)
    return centred * lax.rsqrt(variance + epsilon) * norm_gain


def forward_layer(state, layer_gain, layer_weight):
    normed = normalize(state, layer_gain).astype(jnp.bfloat16)
    preact = jnp.dot(normed, layer_weight, preferred_element_type=jnp.float32)
    return (normed, preact)


def pick(table, index):
    return lax.dynamic_index_in_dim(table, index, 0, keepdims=False)


def place(table, value, index):
    return lax.dynamic_update_index_in_dim(table, value, index, 0)


def per_device(inputs, sample_ids, stored, weight, norm_gain):
    num_sections = lax.axis_size("section")
    section_pos = lax.axis_index("section")
    num_batches, tokens, width = inputs.shape
    rows_total = num_batches * tokens
    layer_weight = weight[0]
    layer_gain = norm_gain[0]
    own_ids = sample_ids[0]
    recv_store = stored[0, 0]
    send_store = stored[0, 1]
    steps_total = num_batches + num_sections - 1
    is_first = section_pos == 0
    is_last = section_pos == num_sections - 1
    loss_scale = 1.0 / math.sqrt(lax.axis_size("dp") * rows_total)
    zero_act = jnp.zeros((tokens, width), jnp.bfloat16)
    stash_init = {
        "states": jnp.zeros((num_batches, tokens, width), jnp.float32),
        "results": jnp.zeros((num_batches, tokens, width), jnp.bfloat16),
    }
    stash_init["normed"] = jnp.zeros((num_batches, tokens, width), jnp.bfloat16)
    stash_init["preact"] = jnp.zeros((num_batches, tokens, width), jnp.float32)

    def forward_step(step, carry):
        incoming, stash = carry
        batch = step - section_pos
        valid = jnp.logical_and(batch >= 0, batch < num_batches)
        slot = jnp.clip(batch, 0, num_batches - 1)
        sample = pick(own_ids, slot)

        def forward_compute(stash_now):
            given = pick(inputs, slot).astype(jnp.float32)
            rebuilt = pick(recv_store, sample).astype(jnp.float32) + incoming.astype(jnp.float32)
            state = jnp.where(is_first, given, rebuilt)
            normed, preact = forward_layer(state, layer_gain, layer_weight)
            result = state + activate(preact)
            reference_copy = pick(send_store, sample).astype(jnp.float32)
            clipped = jnp.clip(result - reference_copy, -delta_bound, delta_bound).astype(
                jnp.bfloat16
            )
            updated = dict(stash_now)
            updated["states"] = place(stash_now["states"], state, slot)
            updated["results"] = place(stash_now["results"], result.astype(jnp.bfloat16), slot)
            updated["normed"] = place(stash_now["normed"], normed, slot)
            updated["preact"] = place(stash_now["preact"], preact, slot)
            return (clipped, updated)

        def forward_skip(stash_now):
            return (zero_act, stash_now)

        clipped, stash = lax.cond(valid, forward_compute, forward_skip, stash)
        outgoing = from_behind(clipped, "section", 1)
        return (outgoing, stash)

    last_incoming, stash = lax.fori_loop(0, steps_total, forward_step, (zero_act, stash_init))
    normed_init = stash["normed"]
    grad_init = jnp.zeros((num_batches, tokens, width), jnp.bfloat16)

    def backward_step(step, carry):
        incoming, normed_buf, grad_buf = carry
        batch = step - (num_sections - 1 - section_pos)
        valid = jnp.logical_and(batch >= 0, batch < num_batches)
        slot = jnp.clip(batch, 0, num_batches - 1)

        def backward_compute(buffers):
            normed_now, grad_now = buffers
            state = pick(stash["states"], slot)
            normed = pick(normed_now, slot)
            preact = pick(stash["preact"], slot)
            result = state + activate(preact)
            upstream = jnp.where(is_last, result * loss_scale, incoming.astype(jnp.float32))
            grad_pre = jax.vjp(activate, preact)[1](upstream)[0].astype(jnp.bfloat16)
            grad_normed = lax.dot_general(
                grad_pre, layer_weight, (((1,), (1,)), ((), ())), preferred_element_type=jnp.float32
            )
            norm_map = partial(normalize, norm_gain=layer_gain)
            grad_state = upstream + jax.vjp(norm_map, state)[1](grad_normed)[0]
            sent = grad_state.astype(jnp.bfloat16)
            return (sent, (place(normed_now, normed, slot), place(grad_now, grad_pre, slot)))

        def backward_skip(buffers):
            return (zero_act, buffers)

        sent, buffers = lax.cond(valid, backward_compute, backward_skip, (normed_buf, grad_buf))
        outgoing = from_behind(sent, "section", -1)
        return (outgoing, buffers[0], buffers[1])

    unused_grad, normed_buf, grad_buf = lax.fori_loop(
        0, steps_total, backward_step, (zero_act, normed_init, grad_init)
    )
    normed_rows = normed_buf.reshape(rows_total, width)
    grad_rows = grad_buf.reshape(rows_total, width)
    replicas = lax.axis_size("dp")
    share = width // replicas
    columns = lax.all_to_all(normed_rows, "dp", split_axis=1, concat_axis=0, tiled=True)
    block_rows = lax.all_gather(grad_rows, "dp", axis=0, tiled=True)
    shard_count = block_rows.shape[0] // rows_total
    cols = columns
    cols = cols.reshape(shard_count, rows_total, share)
    grads_split = block_rows.reshape(shard_count, rows_total, width)
    replica_sums = jnp.einsum(
        "krs,krd->ksd", cols, grads_split, preferred_element_type=jnp.float32
    ).astype(jnp.bfloat16)
    replica_sums = lax.optimization_barrier(replica_sums)
    summed = jnp.sum(replica_sums.astype(jnp.float32), axis=0)
    return (stash["results"][None], summed.astype(jnp.bfloat16)[None])


CORES = 2
MESH = pl.DeviceIdType.MESH
VMEM_LIMIT = 67_043_328


def scope(name):
    return nullcontext()


def step_kernel(
    sections,
    replicas,
    chunk,
    tile,
    parts,
    ids,
    inp_hbm,
    sto_hbm,
    gain,
    w_hbm,
    out_res,
    out_dw,
    inp,
    kept,
    sent,
    w,
    state,
    slope,
    up,
    gn,
    sf,
    rf,
    sb,
    rb,
    nloc,
    nall,
    gall,
    topart,
    frompart,
    in_sem,
    w_sem,
    f_send,
    f_recv,
    b_send,
    b_recv,
    n_send,
    n_recv,
    hub_send,
    mate_send,
    relay_send,
    g_recv,
    p_send,
    p_recv,
):
    rows_total, width = inp.shape
    tokens = sent.shape[1]
    chunks = rows_total // chunk
    tiles = width // tile
    groups = replicas // CORES
    share = width // replicas
    pair = share * CORES
    wide = width // parts
    sub = 16
    subs = chunk // sub
    sec = lax.axis_index("section")
    dp = lax.axis_index("dp")
    z = dp // CORES
    core = dp % CORES
    partner = z * CORES + (1 - core)
    is_last = sec == sections - 1
    not_last = sec < sections - 1
    loss_scale = 1.0 / math.sqrt(replicas * rows_total)
    f32 = jnp.float32
    bf16 = jnp.bfloat16
    half = z // 2
    mate = z + 1 - 2 * lax.rem(z, 2)
    far_hub = 2 - half
    far_first = 2 * (1 - half)
    is_hub = jnp.logical_or(z == 1, z == 2)

    def cols_of(n):
        return pl.ds(pl.multiple_of(n * tile, tile), tile)

    def part_of(p):
        return pl.ds(pl.multiple_of(p * wide, wide), wide)

    def rows_of(c):
        return pl.ds(pl.multiple_of(c * chunk, chunk), chunk)

    def sub_of(c, i):
        return pl.ds(pl.multiple_of(c * chunk + i * sub, sub), sub)

    def peer(d):
        return lax.rem(z + d, groups)

    def at_z(d):
        return {"dp": d * CORES + core}

    def weight_copy(n):
        return pltpu.make_async_copy(w_hbm.at[:, cols_of(n)], w.at[:, cols_of(n)], w_sem.at[n])

    def inp_copy():
        return pltpu.make_async_copy(inp_hbm, inp, in_sem.at[0])

    def kept_copy():
        return pltpu.make_async_copy(sto_hbm.at[0], kept, in_sem.at[1])

    def sent_copy():
        return pltpu.make_async_copy(sto_hbm.at[1], sent, in_sem.at[2])

    def f_copy(c, n):
        return pltpu.make_async_remote_copy(
            src_ref=sf.at[rows_of(c), cols_of(n)],
            dst_ref=rf.at[rows_of(c), cols_of(n)],
            send_sem=f_send.at[c, n],
            recv_sem=f_recv.at[c, n],
            device_id={"section": sec + 1},
            device_id_type=MESH,
        )

    def b_copy(c, i):
        return pltpu.make_async_remote_copy(
            src_ref=sb.at[sub_of(c, i), :],
            dst_ref=rb.at[sub_of(c, i), :],
            send_sem=b_send.at[c, i],
            recv_sem=b_recv.at[c, i],
            device_id={"section": sec - 1},
            device_id_type=MESH,
        )

    def n_copy(c, src, dst):
        return pltpu.make_async_remote_copy(
            src_ref=nloc.at[rows_of(c), pl.ds(pl.multiple_of(dst * pair, 128), pair)],
            dst_ref=nall.at[src, rows_of(c), :],
            send_sem=n_send.at[c, dst],
            recv_sem=n_recv.at[c, src],
            device_id=at_z(dst),
            device_id_type=MESH,
        )

    def g_copy(c, p, src, dst, send_sem):
        return pltpu.make_async_remote_copy(
            src_ref=gall.at[src, rows_of(c), part_of(p)],
            dst_ref=gall.at[src, rows_of(c), part_of(p)],
            send_sem=send_sem,
            recv_sem=g_recv.at[c, src, p],
            device_id=at_z(dst),
            device_id_type=MESH,
        )

    def to_hub(c, p):
        return g_copy(c, p, z, far_hub, hub_send.at[c, p])

    def to_mate(c, p):
        return g_copy(c, p, z, mate, mate_send.at[c, p])

    def relayed(c, p, j):
        return g_copy(c, p, far_first + j, mate, relay_send.at[c, p, j])

    def p_copy(n):
        return pltpu.make_async_remote_copy(
            src_ref=topart.at[:, cols_of(n)],
            dst_ref=frompart.at[:, cols_of(n)],
            send_sem=p_send.at[n],
            recv_sem=p_recv.at[n],
            device_id={"dp": partner},
            device_id_type=MESH,
        )

    barrier = pltpu.get_barrier_semaphore()

    @pl.loop(1, groups)
    def _(d):
        pl.semaphore_signal(barrier, inc=1, device_id=at_z(peer(d)), device_id_type=MESH)

    pl.semaphore_signal(barrier, inc=1, device_id={"dp": partner}, device_id_type=MESH)

    @pl.when(sec > 0)
    def _():
        pl.semaphore_signal(barrier, inc=1, device_id={"section": sec - 1}, device_id_type=MESH)

    @pl.when(not_last)
    def _():
        pl.semaphore_signal(barrier, inc=1, device_id={"section": sec + 1}, device_id_type=MESH)

    inp_copy().start()
    sent_copy().start()

    @pl.loop(0, tiles)
    def _(n):
        weight_copy(n).start()

    kept_copy().start()

    def norm_rows(at):
        values = state[at, :]
        centred = values - jnp.mean(values, axis=-1, keepdims=True)
        variance = jnp.mean(centred * centred, axis=-1, keepdims=True)
        nloc[at, :] = (centred * lax.rsqrt(variance + epsilon) * gain[...]).astype(bf16)

    def first_norm(c):
        @pl.loop(0, subs)
        def _(i):
            at = sub_of(c, i)
            state[at, :] = inp[at, :].astype(f32)
            norm_rows(at)

    inp_copy().wait()

    @pl.when(sec == 0)
    def _():
        first_norm(0)

    sent_copy().wait()

    @pl.when(sec > 0)
    def _():
        kept_copy().wait()

    neighbours = jnp.minimum(sec, 1) + jnp.minimum(sections - 1 - sec, 1)
    with scope("bar"):
        pl.semaphore_wait(barrier, groups + neighbours)

    def forward(c):
        rows = rows_of(c)
        row0 = c * chunk
        slot = row0 // tokens
        off = row0 - slot * tokens
        sid = ids[0, slot]

        @pl.when(jnp.logical_and(sec == 0, c > 0))
        def _():
            first_norm(c)

        @pl.when(sec > 0)
        def _():
            with scope("fwait"):
                @pl.loop(0, tiles)
                def _(n):
                    f_copy(c, n).wait_recv()

            with scope("fnorm"):
                @pl.loop(0, subs)
                def _(i):
                    at = sub_of(c, i)
                    here = pl.ds(pl.multiple_of(off + i * sub, sub), sub)
                    state[at, :] = kept[sid, here, :].astype(f32) + rf[at, :].astype(f32)
                    norm_rows(at)

        @pl.loop(1, groups)
        def _(d):
            n_copy(c, z, peer(d)).start()

        nall[z, rows, :] = nloc[rows, pl.ds(pl.multiple_of(z * pair, 128), pair)]

        with scope("fmm"):
            for n in range(tiles):
                cols = pl.ds(n * tile, tile)

                @pl.when(c == 0)
                def _():
                    weight_copy(n).wait()

                pre = jnp.dot(nloc[rows, :], w[:, cols], preferred_element_type=f32)
                cdf = 0.5 * (1.0 + lax.erf(pre * math.sqrt(0.5)))
                result = state[rows, cols] + pre * cdf
                slope[rows, cols] = cdf + pre * (
                    jnp.exp(-0.5 * pre * pre) * (1.0 / math.sqrt(2.0 * math.pi))
                )
                out_res[rows, cols] = result.astype(bf16)
                up[:, cols] = result * loss_scale
                here = pl.ds(pl.multiple_of(off, chunk), chunk)
                delta = result - sent[sid, here, cols].astype(f32)
                sf[rows, cols] = jnp.clip(delta, -delta_bound, delta_bound).astype(bf16)

                @pl.when(not_last)
                def _():
                    f_copy(c, n).start()

    def backward(c):
        rows = rows_of(c)

        @pl.when(not_last)
        def _():
            with scope("bwait"):
                @pl.loop(0, subs)
                def _(i):
                    b_copy(c, i).wait_recv()
            up[...] = rb[rows, :].astype(f32)

        @pl.loop(0, parts)
        def _(p):
            cols = part_of(p)
            gall[z, rows, cols] = (slope[rows, cols] * up[:, cols]).astype(bf16)
            to_hub(c, p).start()
            to_mate(c, p).start()

        @pl.when(sec > 0)
        def _():
            with scope("bmm"):
                for n in range(tiles):
                    cols = pl.ds(n * tile, tile)
                    turned = lax.dot_general(
                        w[cols, :],
                        gall[z, rows, :],
                        (((1,), (1,)), ((), ())),
                        preferred_element_type=f32,
                    )
                    gn[:, cols] = turned.T

            with scope("bnorm"):
                @pl.loop(0, subs)
                def _(i):
                    at = sub_of(c, i)
                    here = pl.ds(pl.multiple_of(i * sub, sub), sub)
                    values = state[at, :]
                    centred = values - jnp.mean(values, axis=-1, keepdims=True)
                    variance = jnp.mean(centred * centred, axis=-1, keepdims=True)
                    scale = lax.rsqrt(variance + epsilon)
                    unit = centred * scale
                    grad = gn[here, :] * gain[...]
                    first = jnp.mean(grad, axis=-1, keepdims=True)
                    second = jnp.mean(grad * unit, axis=-1, keepdims=True)
                    sb[at, :] = (up[here, :] + scale * (grad - first - unit * second)).astype(bf16)
                    b_copy(c, i).start()

    def relay(c, p):
        @pl.loop(0, 2)
        def _(j):
            relayed(c, p, j).wait_recv()
            relayed(c, p, j).start()

    lag = jnp.where(is_last, 0, jnp.where(sec == sections - 2, chunks // 2 - 1, chunks))
    hold = jnp.where(sec == 0, 1, 3)

    @pl.loop(0, 2 * chunks)
    def _(t):
        @pl.when(t < chunks)
        def _():
            with scope("fwd"):
                forward(t)

        back = t - lag

        @pl.when(jnp.logical_and(back >= 0, back < chunks))
        def _():
            with scope("bwd"):
                backward(back)

            @pl.when(jnp.logical_and(is_hub, back >= hold))
            def _():
                with scope("relay"):
                    @pl.loop(0, parts)
                    def _(p):
                        relay(back - hold, p)

    @pl.loop(0, chunks)
    def _(c):
        @pl.loop(1, groups)
        def _(d):
            n_copy(c, peer(d), z).wait_recv()

    def block(side, n):
        left = nall[:, :, pl.ds(pl.multiple_of(side * share, 128), share)]
        left = left.reshape(groups * rows_total, share)
        right = gall[:, :, cols_of(n)].reshape(groups * rows_total, tile)
        return lax.dot_general(
            left, right, (((0,), (0,)), ((), ())), preferred_element_type=f32
        )

    per_part = wide // tile

    @pl.loop(0, parts)
    def _(p):
        with scope("gwait"):
            @pl.when(is_hub)
            def _():
                @pl.loop(chunks - hold, chunks)
                def _(c):
                    relay(c, p)

            @pl.loop(0, chunks)
            def _(c):
                g_copy(c, p, mate, z, mate_send.at[c, p]).wait_recv()

                @pl.when(jnp.logical_not(is_hub))
                def _():
                    @pl.loop(0, 2)
                    def _(j):
                        g_copy(c, p, far_first + j, z, mate_send.at[c, p]).wait_recv()

        with scope("dw"):
            @pl.loop(0, per_part)
            def _(k):
                n = p * per_part + k
                topart[:, cols_of(n)] = block(1 - core, n).astype(bf16)
                p_copy(n).start()

            @pl.loop(0, per_part)
            def _(k):
                n = p * per_part + k
                own = block(core, n)
                p_copy(n).wait_recv()
                out_dw[:, cols_of(n)] = (own + frompart[:, cols_of(n)].astype(f32)).astype(bf16)

    @pl.when(sec == 0)
    def _():
        kept_copy().wait()

    with scope("drain"):
        @pl.loop(0, tiles)
        def _(n):
            p_copy(n).wait_send()

        @pl.loop(0, chunks)
        def _(c):
            @pl.loop(1, groups)
            def _(d):
                n_copy(c, z, peer(d)).wait_send()

            @pl.loop(0, parts)
            def _(p):
                to_hub(c, p).wait_send()
                to_mate(c, p).wait_send()

                @pl.when(is_hub)
                def _():
                    @pl.loop(0, 2)
                    def _(j):
                        relayed(c, p, j).wait_send()

            @pl.when(not_last)
            def _():
                @pl.loop(0, tiles)
                def _(n):
                    f_copy(c, n).wait_send()

            @pl.when(sec > 0)
            def _():
                @pl.loop(0, subs)
                def _(i):
                    b_copy(c, i).wait_send()


def fused_step(inputs, sample_ids, stored, weight, norm_gain):
    sections = lax.axis_size("section")
    replicas = lax.axis_size("dp")
    batches, tokens, width = inputs.shape
    rows = batches * tokens
    chunk, tile, parts = tokens // 4, 512, 3
    chunks, tiles = rows // chunk, width // tile
    groups = replicas // CORES
    share = width // replicas
    pair = share * CORES
    bf16, f32 = jnp.bfloat16, jnp.float32
    vmem = pl.BlockSpec(memory_space=pltpu.VMEM)
    hbm = pl.BlockSpec(memory_space=pl.ANY)
    dma = pltpu.SemaphoreType.DMA
    subs = chunk // 16
    results, grads = pl.pallas_call(
        partial(step_kernel, sections, replicas, chunk, tile, parts),
        out_shape=(
            jax.ShapeDtypeStruct((rows, width), bf16),
            jax.ShapeDtypeStruct((share, width), bf16),
        ),
        in_specs=[pl.BlockSpec(memory_space=pltpu.SMEM), hbm, hbm, vmem, hbm],
        out_specs=(vmem, vmem),
        scratch_shapes=[
            pltpu.VMEM((rows, width), bf16),
            pltpu.VMEM((batches, tokens, width), bf16),
            pltpu.VMEM((batches, tokens, width), bf16),
            pltpu.VMEM((width, width), bf16),
            pltpu.VMEM((rows, width), f32),
            pltpu.VMEM((rows, width), f32),
            pltpu.VMEM((chunk, width), f32),
            pltpu.VMEM((chunk, width), f32),
            pltpu.VMEM((rows, width), bf16),
            pltpu.VMEM((rows, width), bf16),
            pltpu.VMEM((rows, width), bf16),
            pltpu.VMEM((rows, width), bf16),
            pltpu.VMEM((rows, width), bf16),
            pltpu.VMEM((groups, rows, pair), bf16),
            pltpu.VMEM((groups, rows, width), bf16),
            pltpu.VMEM((share, width), bf16),
            pltpu.VMEM((share, width), bf16),
            dma((3,)),
            dma((tiles,)),
            dma((chunks, tiles)),
            dma((chunks, tiles)),
            dma((chunks, subs)),
            dma((chunks, subs)),
            dma((chunks, groups)),
            dma((chunks, groups)),
            dma((chunks, parts)),
            dma((chunks, parts)),
            dma((chunks, parts, 2)),
            dma((chunks, groups, parts)),
            dma((tiles,)),
            dma((tiles,)),
        ],
        compiler_params=pltpu.CompilerParams(
            collective_id=0, has_side_effects=True, vmem_limit_bytes=VMEM_LIMIT
        ),
    )(sample_ids, inputs.reshape(rows, width), stored[0], norm_gain, weight[0])
    return results.reshape(1, batches, tokens, width), grads[None]


def fits(inputs, replicas):
    batches, tokens, width = inputs.shape
    rows = batches * tokens
    groups = replicas // CORES
    held = 2 * width * width + rows * width * (8 + 2 * (10 + groups)) + 8 * tokens * width
    held += 2 * rows * width + 4 * 2 * width * width // replicas
    aligned = width % 1536 == 0 and tokens % 32 == 0 and replicas == 4 * CORES and (width // replicas) % 128 == 0
    return replicas % CORES == 0 and aligned and held < VMEM_LIMIT


def step(inputs, sample_ids, stored, weight, norm_gain):
    run = fused_step if fits(inputs, lax.axis_size("dp")) else per_device
    return run(inputs, sample_ids, stored, weight, norm_gain)


def solution(mesh):
    return jax.shard_map(
        step,
        mesh=mesh,
        in_specs=(
            P("dp", None, None),
            P("dp", None),
            P("section", None, "dp", None, None),
            P("section", None, None),
            P("section", None),
        ),
        out_specs=(P("section", "dp", None, None), P("section", "dp", None)),
        check_vma=False,
    )
```
